128 devices in a mesh: row: 8 (over x, core), col: 16 (over y, z).
Axes of the slice: x: 4, y: 4, z: 4, core: 2. Of those that a mesh axis runs over, the one named last changes fastest.
Arguments:
- tokens: bfloat16 [65536, 1024], P(('row', 'col')), may hold values from -6 to 6
- expert_ids: int32 [65536, 1], P(('row', 'col')), may hold values from 0 to 127; in each aligned block of 512 rows (0 to 511, 512 to 1023, ...) at most 8 rows name the same one
- gate_prob: float32 [65536], P(('row', 'col')), may hold values from 0.25 to 1
- norm_gain: float32 [1024], replicated, may hold values from 0.1 to 1.9
- weight_in: bfloat16 [128, 1024, 4096], P(('row', 'col')), may hold values from -0.1875 to 0.1875
- weight_out: bfloat16 [128, 4096, 1024], P(('row', 'col')), may hold values from -0.09375 to 0.09375
Outputs:
- mixed: bfloat16 [65536, 1024], P(('row', 'col'))
- routed: int32 [128], P(('row', 'col'))
The draws below stay inside these ranges and needn't reach their ends.
Inputs may be any that keep to these rules, and one draw needn't show every extreme that they name: `expert_ids`: among the 512 tokens of one device no expert is chosen more than 8 times; some expert is chosen exactly 8 times by some device's tokens.
All inputs are finite; a program needn't handle non-finite values.
Results may differ from the reference program's by a relative error of at most 0.001.
The reference program's roundings to bfloat16 on the way (of `normed`, `slots`, `hidden` and `answers`) count: a program that leaves them out, or rounds other values in their place, can miss the bound.
Values may be sent and summed in bfloat16 or wider, within the bound.
No kernel may reach another device: no remote copies, remote signals or barrier semaphores. Data moves between devices by JAX's collectives and lax.ppermute only.
A program may use at most 64 MiB of HBM per device.

```python
import math
import jax
import jax.numpy as jnp
import numpy as np
from jax import lax

D = 1024
FF = 4096
TOK_DEV = 512
EXPERTS = 128
CAP = 8
TOKENS = 65536
DEVICES = 128


def draw_tokens(key, part):
    base_key = jax.random.fold_in(key, 11)
    value_key, sparse_key, choose_key = jax.random.split(base_key, 3)
    values = jnp.clip(jax.random.normal(value_key, (TOKENS, D), jnp.float32), -6.0, 6.0)
    sparse_rows = jax.random.randint(sparse_key, (TOKENS,), 0, 64) == 0
    chosen = jax.random.randint(choose_key, (TOKENS // TOK_DEV,), 0, TOK_DEV)
    position = jnp.arange(TOKENS, dtype=jnp.int32)
    block_index = position // TOK_DEV
    forced_rows = position % TOK_DEV == chosen[block_index]
    kept_rows = jnp.logical_not(jnp.logical_or(sparse_rows, forced_rows)).astype(jnp.float32)
    return (values * kept_rows[:, None]).astype(jnp.bfloat16)


def levels(key, dims, cuts, low, high):
    level, own = 1.0, jax.random.fold_in(key, 6)
    for dim, parts in cuts:
        steps = jnp.exp(jax.random.uniform(jax.random.fold_in(own, dim), (parts,), jnp.float32, low / len(cuts), high / len(cuts)))
        level = level * jnp.repeat(steps, dims[dim] // parts).reshape([-1 if axis == dim else 1 for axis in range(len(dims))])
    return level


def routed_block(own_key, own, number, rows, number_of, top, reach, lean):
    order = jax.random.permutation(own_key, number_of)
    heavy_load, usual = portions_of(number_of, rows * top, reach, lean, True), portions_of(number_of, rows * top, reach, lean, False)
    places = jnp.arange(number_of)

    def named(tallies, offset_by):
        used = int((tallies > 0).sum())
        fixed = max(1, used // 4)
        moved = fixed + (places - fixed + offset_by * (used - fixed)) % max(1, number_of - fixed)
        return jnp.zeros((number_of,), jnp.int32).at[order[jnp.where(places < fixed, places, moved)]].set(jnp.asarray(tallies, jnp.int32))

    tallies = jnp.where(number % 4 == 0, named(heavy_load, number // 4), named(usual, number - number // 4 - 1))
    mixed = jax.random.permutation(jax.random.fold_in(own, 3), number_of)
    donor, sink = mixed[0:number_of // 2 * 2:2], mixed[1:number_of // 2 * 2:2]
    room = jnp.minimum(tallies[donor] - 1, reach - tallies[sink]) // 2
    room = jnp.where((donor == order[0]) | (sink == order[0]) | (tallies[sink] == 0), 0, jnp.maximum(room, 0))
    moved = jax.random.randint(jax.random.fold_in(own, 4), (number_of // 2,), 0, 1 << 20) % (room + 1)
    tallies = tallies.at[donor].add(-moved).at[sink].add(moved)
    labels = jnp.searchsorted(jnp.cumsum(tallies), jnp.arange(rows * top), side="right").astype(jnp.int32)
    table = labels.reshape(top, rows).T
    table = table[jax.random.permutation(jax.random.fold_in(own, 1), rows)]
    offset_by = jax.random.randint(jax.random.fold_in(own, 2), (rows, 1), 0, top)
    return jnp.take_along_axis(table, (jnp.arange(top)[None, :] + offset_by) % top, axis=1)


def portions_of(number_of, total, reach, skew, full):
    weights = [(1 << 20) // math.isqrt(rank ** skew) + 1 for rank in range(1, number_of + 1)]
    largest = reach if full else min(reach, max(-(-total // number_of), total * weights[0] // sum(weights)))
    least = 1 if total - largest >= number_of - 1 else 0
    holding, rest = [largest] + [least] * (number_of - 1), total - largest - least * (number_of - 1)
    while rest > 0:
        candidates = [i for i in range(1, number_of) if holding[i] < largest] or [i for i in range(1, number_of) if holding[i] < reach]
        pool, budget = sum([weights[i] for i in candidates]), rest
        for i in candidates:
            more = min(reach - holding[i], max(1, budget * weights[i] // pool), rest)
            holding[i] = holding[i] + more
            rest = rest - more
    return np.array(holding)


def normal_values(stream_key, dims, width, reach, shards=(), held_as=jnp.bfloat16):
    entries = jax.random.normal(stream_key, dims, jnp.float32) * width
    if len(shards) > 0:
        entries = levels(stream_key, dims, shards, -0.22, 0.18) * entries
    return jnp.clip(entries, min=-reach, max=reach).astype(held_as)


def setup_inputs(seed: int = 0) -> dict:
    seeds = jax.random.split(jax.random.key(seed), 7)
    tokens = draw_tokens(jax.random.fold_in(seeds[6], 71), 0)
    expert_ids_keys = jax.random.split(jax.random.fold_in(seeds[1], 1), TOKENS // TOK_DEV)
    expert_ids_turns = jax.random.permutation(jax.random.fold_in(seeds[1], 3), TOKENS // TOK_DEV)
    expert_ids = jax.vmap(lambda own, number: routed_block(jax.random.fold_in(seeds[1], 2), own, number, TOK_DEV, EXPERTS, 1, CAP, 2))(expert_ids_keys, expert_ids_turns).reshape((TOKENS, 1))
    gate_prob = jnp.clip(0.25 + 0.75 * jax.random.uniform(seeds[2], (TOKENS,), jnp.float32) ** levels(seeds[2], (TOKENS,), ((0, 128),), -0.2, 0.2), 0.25, 1.0)
    norm_gain = jnp.clip(1.0 + 0.18 * jax.random.normal(seeds[3], (D,), jnp.float32), 0.1, 1.9)
    weight_in = normal_values(seeds[4], (EXPERTS, D, FF), D ** -0.5, 0.1875, ((0, 128),))
    weight_out = normal_values(seeds[5], (EXPERTS, FF, D), FF ** -0.5, 0.09375, ((0, 128),))
    return {"tokens": tokens, "expert_ids": expert_ids, "gate_prob": gate_prob, "norm_gain": norm_gain, "weight_in": weight_in, "weight_out": weight_out}


def slot_rank(block_ids):
    count = block_ids.shape[0]
    same = block_ids[:, None] == block_ids[None, :]
    earlier = jnp.arange(count, dtype=jnp.int32)[None, :] < jnp.arange(count, dtype=jnp.int32)[:, None]
    return lax.optimization_barrier(jnp.sum((same & earlier).astype(jnp.int32), axis=1)).astype(jnp.int32)

def expert_ffn(pieces):
    slab, first, second = pieces
    hidden = jnp.maximum(jnp.dot(slab, first, preferred_element_type=jnp.float32), 0.0).astype(jnp.bfloat16)
    return jnp.dot(hidden, second, preferred_element_type=jnp.float32).astype(jnp.bfloat16)

def reference(tokens, expert_ids, gate_prob, norm_gain, weight_in, weight_out):
    flat_ids = expert_ids[:, 0].astype(jnp.int32)
    within = jax.vmap(slot_rank)(flat_ids.reshape(DEVICES, TOK_DEV)).reshape(-1)
    source = (jnp.arange(TOKENS, dtype=jnp.int32) // TOK_DEV).astype(jnp.int32)
    placed = ((flat_ids * DEVICES + source) * CAP + within).astype(jnp.int32)
    wide = tokens.astype(jnp.float32)
    scale = lax.rsqrt(lax.optimization_barrier(jnp.mean(wide * wide, axis=1, keepdims=True)) + 1e-06)
    normed = (wide * scale * norm_gain[None, :]).astype(jnp.bfloat16)
    slots = jnp.zeros((EXPERTS * DEVICES * CAP, D), jnp.bfloat16).at[placed].set(normed)
    slots = slots.reshape(EXPERTS, DEVICES * CAP, D)
    answers = lax.map(expert_ffn, (slots, weight_in, weight_out))
    back = answers.reshape(EXPERTS * DEVICES * CAP, D)[placed]
    mixed = (wide + gate_prob[:, None] * back.astype(jnp.float32)).astype(jnp.bfloat16)
    routed = lax.optimization_barrier(jnp.sum((flat_ids[:, None] == jnp.arange(EXPERTS, dtype=jnp.int32)[None, :]).astype(jnp.int32), axis=0))
    return (mixed, routed)
```

```python
import jax
import jax.numpy as jnp
from jax import lax
from jax.sharding import Mesh
from jax.sharding import PartitionSpec as P

ROW = ("row_0", "row_1")
COL = ("col_0", "col_1")
ROW_COL = ("row_0", "row_1", "col_0", "col_1")
EMPTY = 32768.0


def split_up(array, dim, peers):
    before, after = (array.shape[:dim], array.shape[dim + 1 :])
    return jnp.moveaxis(array.reshape(*before, peers, -1, *after), dim, 0)


def joined_along(parts, dim):
    shape = list(parts.shape[1:])
    shape[dim] *= parts.shape[0]
    return jnp.moveaxis(parts, 0, dim).reshape(shape)


def one_exchange(array, axis, axes, splits, concats):
    sizes = [lax.axis_size(a) for a in axes]
    parts = split_up(array, splits[0], sizes[0])
    parts = jnp.moveaxis(split_up(parts, splits[1] + 1, sizes[1]), 0, 1)
    inside = parts.shape[2:]
    parts = parts.reshape(-1, *inside)
    parts = lax.all_to_all(parts, axis, split_axis=0, concat_axis=0, tiled=True)
    parts = joined_along(parts.reshape(*sizes, *inside), concats[0] + 1)
    return joined_along(parts, concats[1])


def slot_rank(block_ids):
    count = block_ids.shape[0]
    same = block_ids[:, None] == block_ids[None, :]
    earlier = (
        jnp.arange(count, dtype=jnp.int32)[None, :] < jnp.arange(count, dtype=jnp.int32)[:, None]
    )
    return jnp.sum((same & earlier).astype(jnp.int32), axis=1)


def run_expert(received, first, second):
    lead = received.shape[:-1]
    width = received.shape[-1]
    flat_rows = received.reshape(-1, width)
    hidden = jnp.maximum(jnp.dot(flat_rows, first, preferred_element_type=jnp.float32), 0.0).astype(
        jnp.bfloat16
    )
    answer = jnp.dot(hidden, second, preferred_element_type=jnp.float32).astype(jnp.bfloat16)
    return answer.reshape(lead + (width,))


def on_device(tokens, expert_ids, gate_prob, norm_gain, weight_in, weight_out):
    tok_rows, width = tokens.shape
    row_count = lax.axis_size(ROW)
    col_count = lax.axis_size(COL)
    experts = row_count * col_count
    capacity = 2 * tok_rows // experts
    local_ids = expert_ids[:, 0]
    within = slot_rank(local_ids)
    placed = local_ids * capacity + within
    wide = tokens.astype(jnp.float32)
    scale = lax.rsqrt(jnp.mean(wide * wide, axis=1, keepdims=True) + 1e-06)
    normed = (wide * scale * norm_gain[None, :]).astype(jnp.bfloat16)
    table = (placed[None, :] == jnp.arange(experts * capacity, dtype=jnp.int32)[:, None]).astype(
        jnp.bfloat16
    )
    outgoing = jnp.dot(table, normed, preferred_element_type=jnp.float32).astype(jnp.bfloat16)
    taken = jnp.sum(
        (local_ids[:, None] == jnp.arange(experts, dtype=jnp.int32)[None, :]).astype(jnp.int32),
        axis=0,
    )
    empty = jnp.arange(capacity, dtype=jnp.int32)[None, :] >= taken[:, None]
    empty = empty.reshape(-1)[:, None] & (jnp.arange(width, dtype=jnp.int32)[None, :] < 128)
    outgoing = jnp.where(empty, jnp.bfloat16(EMPTY), outgoing)
    first = weight_in[0]
    second = weight_out[0]
    grid_out = outgoing.reshape(row_count, col_count, capacity, width)
    arrived = one_exchange(grid_out, ROW_COL, (ROW, COL), (0, 1), (0, 1))
    marks = arrived[..., 0].astype(jnp.float32)
    routed = jnp.sum((marks < 0.5 * EMPTY).astype(jnp.int32)).reshape(1)
    answers = run_expert(arrived, first, second)
    returned = one_exchange(answers, ROW_COL, (ROW, COL), (0, 1), (0, 1))
    returned = returned.reshape(experts * capacity, width)
    back = jnp.einsum("st,sd->td", table, returned, preferred_element_type=jnp.float32)
    mixed = (wide + gate_prob[:, None] * back).astype(jnp.bfloat16)
    return (mixed, routed)


def solution(mesh):
    finer = Mesh(mesh.devices.reshape(4, 2, 4, 4), ("row_0", "row_1", "col_0", "col_1"))
    return jax.shard_map(
        on_device,
        mesh=finer,
        in_specs=(
            P(ROW_COL, None),
            P(ROW_COL, None),
            P(ROW_COL),
            P(),
            P(ROW_COL, None, None),
            P(ROW_COL, None, None),
        ),
        out_specs=(P(ROW_COL, None), P(ROW_COL)),
        check_vma=False,
    )
```

```python
import jax
import jax.numpy as jnp
from jax import lax
from jax.experimental import pallas as pl
from jax.experimental.pallas import tpu as pltpu
from jax.sharding import Mesh
from jax.sharding import PartitionSpec as P

ROW_COL = ("row_0", "row_1", "col_0", "col_1")
EMPTY = 32768.0
MARKED = 128
DISPATCH_COLS = 256
FF_BLOCK = 512
COMBINE_COLS = 256


def one_hot(match):
    return jnp.where(match, 1.0, 0.0).astype(jnp.bfloat16)


def dispatch_kernel(tok_ref, ids_ref, gain_ref, out_ref, placed_ref, table_ref, normed_ref):
    slots, count = table_ref.shape
    cols = out_ref.shape[1]
    step = pl.program_id(0)

    @pl.when(step == 0)
    def _():
        ids = ids_ref[...]
        experts = 128
        capacity = slots // experts
        match = lax.broadcasted_iota(jnp.int32, (experts, count), 0) == ids
        before = lax.broadcasted_iota(jnp.int32, (count, count), 0) < lax.broadcasted_iota(
            jnp.int32, (count, count), 1
        )
        earlier = jnp.dot(one_hot(match), one_hot(before), preferred_element_type=jnp.float32)
        within = jnp.sum(jnp.where(match, earlier, 0.0), axis=0, keepdims=True)
        placed = ids * capacity + within.astype(jnp.int32)
        placed_ref[...] = placed
        table_ref[...] = one_hot(lax.broadcasted_iota(jnp.int32, (slots, count), 0) == placed)
        wide = tok_ref[...].astype(jnp.float32)
        scale = lax.rsqrt(jnp.mean(wide * wide, axis=1, keepdims=True) + 1e-06)
        normed_ref[...] = (wide * scale * gain_ref[...]).astype(jnp.bfloat16)

    table = table_ref[...]
    start = pl.multiple_of(step * cols, cols)
    sent = jnp.dot(table, normed_ref[:, pl.ds(start, cols)], preferred_element_type=jnp.float32)
    out_ref[...] = sent.astype(jnp.bfloat16)

    @pl.when(step == 0)
    def _():
        filled = jnp.dot(
            table, jnp.ones((count, MARKED), jnp.bfloat16), preferred_element_type=jnp.float32
        )
        out_ref[:, :MARKED] = jnp.where(filled > 0.5, sent[:, :MARKED], EMPTY).astype(jnp.bfloat16)


def dispatch(tokens, ids, gain, slots):
    count, width = tokens.shape
    cols = DISPATCH_COLS
    return pl.pallas_call(
        dispatch_kernel,
        grid=(width // cols,),
        in_specs=[
            pl.BlockSpec((count, width), lambda j: (0, 0)),
            pl.BlockSpec((1, count), lambda j: (0, 0)),
            pl.BlockSpec((1, width), lambda j: (0, 0)),
        ],
        out_specs=[
            pl.BlockSpec((slots, cols), lambda j: (0, j)),
            pl.BlockSpec((1, count), lambda j: (0, 0)),
        ],
        out_shape=[
            jax.ShapeDtypeStruct((slots, width), jnp.bfloat16),
            jax.ShapeDtypeStruct((1, count), jnp.int32),
        ],
        scratch_shapes=[
            pltpu.VMEM((slots, count), jnp.bfloat16),
            pltpu.VMEM((count, width), jnp.bfloat16),
        ],
        cost_estimate=pl.CostEstimate(
            flops=2 * slots * count * width, bytes_accessed=4 * slots * width, transcendentals=0
        ),
        name="dispatch",
    )(tokens, ids, gain)


def prepare_kernel(placed_ref, gate_ref, table_ref, gates_ref):
    count, slots = table_ref.shape
    lanes = gates_ref.shape[1]
    rows = jnp.broadcast_to(placed_ref[...].astype(jnp.float32), (lanes, count)).T.astype(jnp.int32)
    gates_ref[...] = jnp.broadcast_to(gate_ref[...], (lanes, count)).T
    lane = lax.broadcasted_iota(jnp.int32, (count, lanes), 1)
    for start in range(0, slots, lanes):
        table_ref[:, start : start + lanes] = one_hot(lane + start == rows)


def prepare(placed, gate, slots):
    count = placed.shape[1]
    return pl.pallas_call(
        prepare_kernel,
        out_shape=[
            jax.ShapeDtypeStruct((count, slots), jnp.bfloat16),
            jax.ShapeDtypeStruct((count, 128), jnp.float32),
        ],
        cost_estimate=pl.CostEstimate(
            flops=4 * slots * count, bytes_accessed=2 * slots * count, transcendentals=0
        ),
        name="prepare",
    )(placed, gate)


def expert_kernel(x_ref, first_ref, second_ref, out_ref, routed_ref, total_ref):
    step = pl.program_id(0)

    @pl.when(step == 0)
    def _():
        kept = jnp.where(x_ref[:, :MARKED].astype(jnp.float32) < 0.5 * EMPTY, 1.0, 0.0)
        routed_ref[0] = jnp.sum(kept).astype(jnp.int32) // MARKED

    hidden = jnp.maximum(
        jnp.dot(x_ref[...], first_ref[...], preferred_element_type=jnp.float32), 0.0
    ).astype(jnp.bfloat16)
    part = jnp.dot(hidden, second_ref[...], preferred_element_type=jnp.float32)

    @pl.when(step == 0)
    def _():
        total_ref[...] = part

    @pl.when((step > 0) & (step < pl.num_programs(0) - 1))
    def _():
        total_ref[...] += part

    @pl.when(step == pl.num_programs(0) - 1)
    def _():
        out_ref[...] = (total_ref[...] + part).astype(jnp.bfloat16)


def expert(x, first, second):
    rows, width = x.shape
    ff = first.shape[1]
    return pl.pallas_call(
        expert_kernel,
        grid=(ff // FF_BLOCK,),
        in_specs=[
            pl.BlockSpec((rows, width), lambda j: (0, 0)),
            pl.BlockSpec((width, FF_BLOCK), lambda j: (0, j)),
            pl.BlockSpec((FF_BLOCK, width), lambda j: (j, 0)),
        ],
        out_specs=[
            pl.BlockSpec((rows, width), lambda j: (0, 0)),
            pl.BlockSpec(memory_space=pltpu.SMEM),
        ],
        out_shape=[
            jax.ShapeDtypeStruct((rows, width), jnp.bfloat16),
            jax.ShapeDtypeStruct((1,), jnp.int32),
        ],
        scratch_shapes=[pltpu.VMEM((rows, width), jnp.float32)],
        cost_estimate=pl.CostEstimate(
            flops=4 * rows * width * ff, bytes_accessed=4 * width * (ff + rows), transcendentals=0
        ),
        name="expert",
    )(x, first, second)


def combine_kernel(table_ref, back_ref, gates_ref, tok_ref, out_ref):
    back = jnp.dot(table_ref[...], back_ref[...], preferred_element_type=jnp.float32)
    gates = jnp.concatenate([gates_ref[...]] * (back.shape[1] // gates_ref.shape[1]), axis=1)
    out_ref[...] = (tok_ref[...].astype(jnp.float32) + gates * back).astype(jnp.bfloat16)


def combine(table, back, gates, tokens):
    count, width = tokens.shape
    slots = back.shape[0]
    cols = COMBINE_COLS
    return pl.pallas_call(
        combine_kernel,
        grid=(width // cols,),
        in_specs=[
            pl.BlockSpec((count, slots), lambda j: (0, 0)),
            pl.BlockSpec((slots, cols), lambda j: (0, j)),
            pl.BlockSpec(gates.shape, lambda j: (0, 0)),
            pl.BlockSpec((count, cols), lambda j: (0, j)),
        ],
        out_specs=pl.BlockSpec((count, cols), lambda j: (0, j)),
        out_shape=jax.ShapeDtypeStruct((count, width), jnp.bfloat16),
        cost_estimate=pl.CostEstimate(
            flops=2 * slots * count * width, bytes_accessed=4 * slots * width, transcendentals=0
        ),
        name="combine",
    )(table, back, gates, tokens)


def exchange(rows, devices):
    parts = rows.reshape(devices, rows.shape[0] // devices, rows.shape[1])
    parts = lax.all_to_all(parts, ROW_COL, split_axis=0, concat_axis=0, tiled=True)
    return parts.reshape(rows.shape)


def on_device(tokens, expert_ids, gate_prob, norm_gain, weight_in, weight_out):
    tok_rows, width = tokens.shape
    experts = lax.axis_size(ROW_COL)
    slots = 2 * tok_rows
    ids = expert_ids.reshape(1, tok_rows)
    outgoing, placed = dispatch(tokens, ids, norm_gain.reshape(1, width), slots)
    arrived = exchange(outgoing, experts)
    table, gates = prepare(placed, gate_prob.reshape(1, tok_rows), slots)
    answers, routed = expert(arrived, weight_in[0], weight_out[0])
    returned = exchange(answers, experts)
    mixed = combine(table, returned, gates, tokens)
    return (mixed, routed)


def solution(mesh):
    finer = Mesh(mesh.devices.reshape(4, 2, 4, 4), ROW_COL)
    return jax.shard_map(
        on_device,
        mesh=finer,
        in_specs=(
            P(ROW_COL, None),
            P(ROW_COL, None),
            P(ROW_COL),
            P(),
            P(ROW_COL, None, None),
            P(ROW_COL, None, None),
        ),
        out_specs=(P(ROW_COL, None), P(ROW_COL)),
        check_vma=False,
    )
```

```python
import jax
import jax.numpy as jnp
from jax import lax
from jax.experimental import pallas as pl
from jax.experimental.pallas import tpu as pltpu
from jax.sharding import Mesh
from jax.sharding import PartitionSpec as P

ROW_COL = ("row_0", "row_1", "col_0", "col_1")
EMPTY = 32768.0
MARKED = 128
DISPATCH_COLS = 256
HIDDEN_COLS = 1024
ANSWER_COLS = 512
COMBINE_COLS = 512
VMEM_LIMIT = 50 << 20

HBM = pl.BlockSpec(memory_space=pltpu.HBM)
VMEM = pl.BlockSpec(memory_space=pltpu.VMEM)
SMEM = pl.BlockSpec(memory_space=pltpu.SMEM)


def one_hot(match):
    return jnp.where(match, 1.0, 0.0).astype(jnp.bfloat16)


def columns(block, size):
    start = block * size
    return pl.ds(start if isinstance(block, int) else pl.multiple_of(start, size), size)


def dispatch_kernel(
    tok_hbm, ids_hbm, gain_hbm, out_hbm, placed_ref, tok_ref, ids_ref, gain_ref, sent_ref, in_sem, out_sem
):
    count, width = tok_ref.shape
    blocks, slots, cols = sent_ref.shape
    experts = 128
    capacity = slots // experts
    ids_copy = pltpu.make_async_copy(ids_hbm, ids_ref, in_sem.at[0])
    tok_copy = pltpu.make_async_copy(tok_hbm, tok_ref, in_sem.at[1])
    gain_copy = pltpu.make_async_copy(gain_hbm, gain_ref, in_sem.at[2])
    ids_copy.start()
    tok_copy.start()
    gain_copy.start()
    before = lax.broadcasted_iota(jnp.int32, (count, count), 0) < lax.broadcasted_iota(
        jnp.int32, (count, count), 1
    )
    ids_copy.wait()
    ids = ids_ref[...]
    match = lax.broadcasted_iota(jnp.int32, (experts, count), 0) == ids
    earlier = jnp.dot(one_hot(match), one_hot(before), preferred_element_type=jnp.float32)
    within = jnp.sum(jnp.where(match, earlier, 0.0), axis=0, keepdims=True)
    placed = ids * capacity + within.astype(jnp.int32)
    placed_ref[...] = placed
    table = one_hot(lax.broadcasted_iota(jnp.int32, (slots, count), 0) == placed)
    filled = jnp.dot(
        table, jnp.ones((count, MARKED), jnp.bfloat16), preferred_element_type=jnp.float32
    )
    tok_copy.wait()
    gain_copy.wait()
    wide = tok_ref[...].astype(jnp.float32)
    scale = lax.rsqrt(jnp.mean(wide * wide, axis=1, keepdims=True) + 1e-06)
    normed = (wide * scale * gain_ref[...]).astype(jnp.bfloat16)
    copies = []
    for block in range(blocks):
        sent = jnp.dot(
            table, normed[:, block * cols : (block + 1) * cols], preferred_element_type=jnp.float32
        )
        if block == 0:
            sent_ref[block, :, :MARKED] = jnp.where(filled > 0.5, sent[:, :MARKED], EMPTY).astype(
                jnp.bfloat16
            )
            sent_ref[block, :, MARKED:] = sent[:, MARKED:].astype(jnp.bfloat16)
        else:
            sent_ref[block] = sent.astype(jnp.bfloat16)
        copies.append(
            pltpu.make_async_copy(
                sent_ref.at[block], out_hbm.at[:, columns(block, cols)], out_sem.at[block]
            )
        )
        copies[-1].start()
    for copy in copies:
        copy.wait()


def dispatch(tokens, ids, gain, slots):
    count, width = tokens.shape
    blocks = width // DISPATCH_COLS
    return pl.pallas_call(
        dispatch_kernel,
        in_specs=[HBM, HBM, HBM],
        out_specs=[HBM, VMEM],
        out_shape=[
            pltpu.HBM((slots, width), jnp.bfloat16),
            jax.ShapeDtypeStruct((1, count), jnp.int32),
        ],
        scratch_shapes=[
            pltpu.VMEM((count, width), jnp.bfloat16),
            pltpu.VMEM((1, count), jnp.int32),
            pltpu.VMEM((1, width), jnp.float32),
            pltpu.VMEM((blocks, slots, DISPATCH_COLS), jnp.bfloat16),
            pltpu.SemaphoreType.DMA((3,)),
            pltpu.SemaphoreType.DMA((blocks,)),
        ],
        compiler_params=pltpu.CompilerParams(vmem_limit_bytes=VMEM_LIMIT),
        cost_estimate=pl.CostEstimate(
            flops=2 * slots * count * width, bytes_accessed=4 * slots * width, transcendentals=0
        ),
        name="dispatch",
    )(tokens, ids, gain)


def prepare_kernel(placed_ref, gate_ref, table_ref, gates_ref):
    count, slots = table_ref.shape
    lanes = gates_ref.shape[1]
    rows = jnp.broadcast_to(placed_ref[...].astype(jnp.float32), (lanes, count)).T.astype(jnp.int32)
    gates_ref[...] = jnp.broadcast_to(gate_ref[...], (lanes, count)).T
    lane = lax.broadcasted_iota(jnp.int32, (count, lanes), 1)
    for start in range(0, slots, lanes):
        table_ref[:, start : start + lanes] = one_hot(lane + start == rows)


def prepare(placed, gate, slots):
    count = placed.shape[1]
    return pl.pallas_call(
        prepare_kernel,
        out_shape=[
            jax.ShapeDtypeStruct((count, slots), jnp.bfloat16),
            jax.ShapeDtypeStruct((count, 128), jnp.float32),
        ],
        compiler_params=pltpu.CompilerParams(vmem_limit_bytes=16 << 20),
        cost_estimate=pl.CostEstimate(
            flops=4 * slots * count, bytes_accessed=2 * slots * count, transcendentals=0
        ),
        name="prepare",
    )(placed, gate)


def expert_kernel(
    x_ref, first_hbm, second_hbm, out_hbm, routed_ref,
    first_ref, second_ref, hidden_ref, answer_ref, in_sem, out_sem,
):
    hidden_blocks, _, hidden_cols = first_ref.shape
    answer_blocks, _, answer_cols = second_ref.shape

    def first_copy(block):
        return pltpu.make_async_copy(
            first_hbm.at[:, columns(block, hidden_cols)], first_ref.at[block], in_sem.at[0, block]
        )

    def second_copy(block):
        return pltpu.make_async_copy(
            second_hbm.at[:, columns(block, answer_cols)], second_ref.at[block], in_sem.at[1, block]
        )

    def answer_copy(block):
        return pltpu.make_async_copy(
            answer_ref.at[block], out_hbm.at[:, columns(block, answer_cols)], out_sem.at[block]
        )

    for block in range(hidden_blocks):
        first_copy(block).start()
    for block in range(answer_blocks):
        second_copy(block).start()
    kept = jnp.where(x_ref[:, :MARKED].astype(jnp.float32) < 0.5 * EMPTY, 1.0, 0.0)
    routed_ref[0] = jnp.sum(kept).astype(jnp.int32) // MARKED

    @pl.loop(0, hidden_blocks)
    def _(block):
        first_copy(block).wait()
        hidden = jnp.dot(x_ref[...], first_ref[block], preferred_element_type=jnp.float32)
        hidden_ref[:, columns(block, hidden_cols)] = jnp.maximum(hidden, 0.0).astype(jnp.bfloat16)

    @pl.loop(0, answer_blocks)
    def _(block):
        second_copy(block).wait()
        answer = jnp.dot(hidden_ref[...], second_ref[block], preferred_element_type=jnp.float32)
        answer_ref[block] = answer.astype(jnp.bfloat16)
        answer_copy(block).start()

    for block in range(answer_blocks):
        answer_copy(block).wait()


def expert(x, first, second):
    rows, width = x.shape
    ff = first.shape[1]
    hidden_blocks, answer_blocks = ff // HIDDEN_COLS, width // ANSWER_COLS
    return pl.pallas_call(
        expert_kernel,
        in_specs=[VMEM, HBM, HBM],
        out_specs=[HBM, SMEM],
        out_shape=[
            pltpu.HBM((rows, width), jnp.bfloat16),
            jax.ShapeDtypeStruct((1,), jnp.int32),
        ],
        scratch_shapes=[
            pltpu.VMEM((hidden_blocks, width, HIDDEN_COLS), jnp.bfloat16),
            pltpu.VMEM((answer_blocks, ff, ANSWER_COLS), jnp.bfloat16),
            pltpu.VMEM((rows, ff), jnp.bfloat16),
            pltpu.VMEM((answer_blocks, rows, ANSWER_COLS), jnp.bfloat16),
            pltpu.SemaphoreType.DMA((2, max(hidden_blocks, answer_blocks))),
            pltpu.SemaphoreType.DMA((answer_blocks,)),
        ],
        compiler_params=pltpu.CompilerParams(vmem_limit_bytes=VMEM_LIMIT),
        cost_estimate=pl.CostEstimate(
            flops=4 * rows * width * ff, bytes_accessed=4 * width * (ff + rows), transcendentals=0
        ),
        name="expert",
    )(x, first, second)


def combine_kernel(
    table_ref, back_ref, gates_ref, tok_hbm, out_hbm, tok_ref, mixed_ref, tok_sem, out_sem
):
    blocks, _, cols = mixed_ref.shape
    tok_copy = pltpu.make_async_copy(tok_hbm, tok_ref, tok_sem)
    tok_copy.start()
    gates = jnp.concatenate([gates_ref[...]] * (cols // gates_ref.shape[1]), axis=1)
    copies = []
    for block in range(blocks):
        span = slice(block * cols, (block + 1) * cols)
        back = jnp.dot(table_ref[...], back_ref[:, span], preferred_element_type=jnp.float32)
        if block == 0:
            tok_copy.wait()
        mixed = tok_ref[:, span].astype(jnp.float32) + gates * back
        mixed_ref[block] = mixed.astype(jnp.bfloat16)
        copies.append(
            pltpu.make_async_copy(
                mixed_ref.at[block], out_hbm.at[:, columns(block, cols)], out_sem.at[block]
            )
        )
        copies[-1].start()
    for copy in copies:
        copy.wait()


def combine(table, back, gates, tokens):
    count, width = tokens.shape
    slots = back.shape[0]
    blocks = width // COMBINE_COLS
    return pl.pallas_call(
        combine_kernel,
        in_specs=[VMEM, VMEM, VMEM, HBM],
        out_specs=HBM,
        out_shape=jax.ShapeDtypeStruct((count, width), jnp.bfloat16),
        scratch_shapes=[
            pltpu.VMEM((count, width), jnp.bfloat16),
            pltpu.VMEM((blocks, count, COMBINE_COLS), jnp.bfloat16),
            pltpu.SemaphoreType.DMA,
            pltpu.SemaphoreType.DMA((blocks,)),
        ],
        compiler_params=pltpu.CompilerParams(vmem_limit_bytes=16 << 20),
        cost_estimate=pl.CostEstimate(
            flops=2 * slots * count * width, bytes_accessed=4 * slots * width, transcendentals=0
        ),
        name="combine",
    )(table, back, gates, tokens)


def exchange(rows, devices):
    parts = rows.reshape(devices, rows.shape[0] // devices, rows.shape[1])
    parts = lax.all_to_all(parts, ROW_COL, split_axis=0, concat_axis=0, tiled=True)
    return parts.reshape(rows.shape)


def on_device(tokens, expert_ids, gate_prob, norm_gain, weight_in, weight_out):
    tok_rows, width = tokens.shape
    experts = lax.axis_size(ROW_COL)
    slots = 2 * tok_rows
    tokens = pltpu.with_memory_space_constraint(tokens, pltpu.HBM)
    ids = pltpu.with_memory_space_constraint(expert_ids.reshape(1, tok_rows), pltpu.HBM)
    gain = pltpu.with_memory_space_constraint(norm_gain.reshape(1, width), pltpu.HBM)
    outgoing, placed = dispatch(tokens, ids, gain, slots)
    arrived = exchange(outgoing, experts)
    table, gates = prepare(placed, gate_prob.reshape(1, tok_rows), slots)
    answers, routed = expert(arrived, weight_in[0], weight_out[0])
    returned = exchange(answers, experts)
    mixed = combine(table, returned, gates, tokens)
    return (mixed, routed)


def solution(mesh):
    finer = Mesh(mesh.devices.reshape(4, 2, 4, 4), ROW_COL)
    return jax.shard_map(
        on_device,
        mesh=finer,
        in_specs=(
            P(ROW_COL, None),
            P(ROW_COL, None),
            P(ROW_COL),
            P(),
            P(ROW_COL, None, None),
            P(ROW_COL, None, None),
        ),
        out_specs=(P(ROW_COL, None), P(ROW_COL)),
        check_vma=False,
    )
```

```python
import jax
import jax.numpy as jnp
from jax import lax
from jax.experimental import pallas as pl
from jax.experimental.pallas import tpu as pltpu
from jax.sharding import Mesh
from jax.sharding import PartitionSpec as P

ROW_COL = ("row_0", "row_1", "col_0", "col_1")
EMPTY = 32768.0
MARKED = 128
DISPATCH_COLS = 256
HEAD_COLS = 512
HIDDEN_COLS = 512
ANSWER_COLS = 512
COMBINE_COLS = 512
VMEM_LIMIT = 44 << 20

HBM = pl.BlockSpec(memory_space=pltpu.HBM)
VMEM = pl.BlockSpec(memory_space=pltpu.VMEM)
SMEM = pl.BlockSpec(memory_space=pltpu.SMEM)


def one_hot(match):
    return jnp.where(match, 1.0, 0.0).astype(jnp.bfloat16)


def columns(block, size, offset=0):
    start = block * size + offset
    return pl.ds(start if isinstance(block, int) else pl.multiple_of(start, 128), size)


def dispatch_kernel(
    tok_hbm, ids_hbm, gain_hbm, first_hbm, out_ref, placed_ref, head_ref,
    tok_ref, ids_ref, gain_ref, in_sem,
):
    count, width = tok_ref.shape
    slots, cols = out_ref.shape[0], DISPATCH_COLS
    experts = 128
    capacity = slots // experts
    ids_copy = pltpu.make_async_copy(ids_hbm, ids_ref, in_sem.at[0])
    tok_copy = pltpu.make_async_copy(tok_hbm, tok_ref, in_sem.at[1])
    gain_copy = pltpu.make_async_copy(gain_hbm, gain_ref, in_sem.at[2])
    ids_copy.start()
    tok_copy.start()
    gain_copy.start()
    head_copy = pltpu.make_async_copy(
        first_hbm.at[:, pl.ds(0, head_ref.shape[1])], head_ref, in_sem.at[3]
    )
    head_copy.start()
    before = lax.broadcasted_iota(jnp.int32, (count, count), 0) < lax.broadcasted_iota(
        jnp.int32, (count, count), 1
    )
    ids_copy.wait()
    ids = ids_ref[...]
    match = lax.broadcasted_iota(jnp.int32, (experts, count), 0) == ids
    earlier = jnp.dot(one_hot(match), one_hot(before), preferred_element_type=jnp.float32)
    within = jnp.sum(jnp.where(match, earlier, 0.0), axis=0, keepdims=True)
    placed = ids * capacity + within.astype(jnp.int32)
    placed_ref[...] = placed
    table = one_hot(lax.broadcasted_iota(jnp.int32, (slots, count), 0) == placed)
    filled = jnp.dot(
        table, jnp.ones((count, MARKED), jnp.bfloat16), preferred_element_type=jnp.float32
    )
    tok_copy.wait()
    gain_copy.wait()
    wide = tok_ref[...].astype(jnp.float32)
    scale = lax.rsqrt(jnp.mean(wide * wide, axis=1, keepdims=True) + 1e-06)
    normed = (wide * scale * gain_ref[...]).astype(jnp.bfloat16)
    for start in range(0, width, cols):
        sent = jnp.dot(
            table, normed[:, start : start + cols], preferred_element_type=jnp.float32
        )
        if start == 0:
            marked = jnp.where(filled > 0.5, sent[:, :MARKED], EMPTY).astype(jnp.bfloat16)
            out_ref[:, :MARKED] = marked
            out_ref[:, MARKED:cols] = sent[:, MARKED:].astype(jnp.bfloat16)
        else:
            out_ref[:, start : start + cols] = sent.astype(jnp.bfloat16)
    head_copy.wait()


def dispatch(tokens, ids, gain, first, slots):
    count, width = tokens.shape
    return pl.pallas_call(
        dispatch_kernel,
        in_specs=[HBM, HBM, HBM, HBM],
        out_specs=[VMEM, VMEM, VMEM],
        out_shape=[
            pltpu.VMEM((slots, width), jnp.bfloat16),
            jax.ShapeDtypeStruct((1, count), jnp.int32),
            pltpu.VMEM((first.shape[0], HEAD_COLS), jnp.bfloat16),
        ],
        scratch_shapes=[
            pltpu.VMEM((count, width), jnp.bfloat16),
            pltpu.VMEM((1, count), jnp.int32),
            pltpu.VMEM((1, width), jnp.float32),
            pltpu.SemaphoreType.DMA((4,)),
        ],
        compiler_params=pltpu.CompilerParams(vmem_limit_bytes=VMEM_LIMIT),
        cost_estimate=pl.CostEstimate(
            flops=2 * slots * count * width, bytes_accessed=4 * slots * width, transcendentals=0
        ),
        name="dispatch",
    )(tokens, ids, gain, first)


def expert_kernel(
    x_ref, head_ref, placed_ref, gate_ref, first_hbm, second_hbm, tok_hbm,
    out_ref, routed_ref, table_ref, gates_ref, tok_ref,
    first_ref, second_ref, hidden_ref, rows_ref, in_sem, tok_sem,
):
    hidden_blocks, _, hidden_cols = first_ref.shape
    answer_blocks, _, answer_cols = second_ref.shape
    head_cols = head_ref.shape[1]

    def first_copy(block):
        return pltpu.make_async_copy(
            first_hbm.at[:, columns(block, hidden_cols, head_cols)],
            first_ref.at[block],
            in_sem.at[0, block],
        )

    def second_copy(block):
        return pltpu.make_async_copy(
            second_hbm.at[:, columns(block, answer_cols)], second_ref.at[block], in_sem.at[1, block]
        )

    tok_copy = pltpu.make_async_copy(tok_hbm, tok_ref, tok_sem)
    for block in range(hidden_blocks):
        first_copy(block).start()
    for block in range(answer_blocks):
        second_copy(block).start()
    tok_copy.start()
    kept = jnp.where(x_ref[:, :MARKED].astype(jnp.float32) < 0.5 * EMPTY, 1.0, 0.0)
    routed_ref[0] = jnp.sum(kept).astype(jnp.int32) // MARKED

    count, lanes = rows_ref.shape
    placed = jnp.broadcast_to(placed_ref[...].astype(jnp.float32), (lanes, count))
    rows_ref[...] = placed.T.astype(jnp.int32)
    gates_ref[...] = jnp.broadcast_to(gate_ref[...], (lanes, count)).T

    def combine_columns(block):
        lane = lax.broadcasted_iota(jnp.int32, (count, lanes), 1) + block * lanes
        table_ref[:, columns(block, lanes)] = one_hot(lane == rows_ref[...])

    combine_columns(hidden_blocks)
    head = jnp.dot(x_ref[...], head_ref[...], preferred_element_type=jnp.float32)
    hidden_ref[:, :head_cols] = jnp.maximum(head, 0.0).astype(jnp.bfloat16)

    @pl.loop(0, hidden_blocks)
    def _(block):
        first_copy(block).wait()
        combine_columns(block)
        hidden = jnp.dot(x_ref[...], first_ref[block], preferred_element_type=jnp.float32)
        hidden_ref[:, columns(block, hidden_cols, head_cols)] = jnp.maximum(hidden, 0.0).astype(
            jnp.bfloat16
        )

    @pl.loop(0, answer_blocks)
    def _(block):
        second_copy(block).wait()
        answer = jnp.dot(hidden_ref[...], second_ref[block], preferred_element_type=jnp.float32)
        out_ref[:, columns(block, answer_cols)] = answer.astype(jnp.bfloat16)

    tok_copy.wait()


def expert(x, head, placed, gate, first, second, tokens):
    rows, width = x.shape
    ff = first.shape[1]
    hidden_blocks, answer_blocks = (ff - HEAD_COLS) // HIDDEN_COLS, width // ANSWER_COLS
    return pl.pallas_call(
        expert_kernel,
        in_specs=[VMEM, VMEM, VMEM, VMEM, HBM, HBM, HBM],
        out_specs=[VMEM, SMEM, VMEM, VMEM, VMEM],
        out_shape=[
            pltpu.VMEM((rows, width), jnp.bfloat16),
            jax.ShapeDtypeStruct((1,), jnp.int32),
            pltpu.VMEM((placed.shape[1], rows), jnp.bfloat16),
            pltpu.VMEM((placed.shape[1], 128), jnp.float32),
            pltpu.VMEM(tokens.shape, jnp.bfloat16),
        ],
        scratch_shapes=[
            pltpu.VMEM((hidden_blocks, width, HIDDEN_COLS), jnp.bfloat16),
            pltpu.VMEM((answer_blocks, ff, ANSWER_COLS), jnp.bfloat16),
            pltpu.VMEM((rows, ff), jnp.bfloat16),
            pltpu.VMEM((placed.shape[1], 128), jnp.int32),
            pltpu.SemaphoreType.DMA((2, max(hidden_blocks, answer_blocks))),
            pltpu.SemaphoreType.DMA,
        ],
        compiler_params=pltpu.CompilerParams(vmem_limit_bytes=VMEM_LIMIT),
        cost_estimate=pl.CostEstimate(
            flops=4 * rows * width * ff, bytes_accessed=4 * width * (ff + rows), transcendentals=0
        ),
        name="expert",
    )(x, head, placed, gate, first, second, tokens)


def combine_kernel(
    table_ref, back_ref, gates_ref, tok_ref, out_hbm, mixed_ref, out_sem
):
    blocks, _, cols = mixed_ref.shape
    gates = jnp.concatenate([gates_ref[...]] * (cols // gates_ref.shape[1]), axis=1)
    copies = []
    for block in range(blocks):
        span = slice(block * cols, (block + 1) * cols)
        back = jnp.dot(table_ref[...], back_ref[:, span], preferred_element_type=jnp.float32)
        mixed = tok_ref[:, span].astype(jnp.float32) + gates * back
        mixed_ref[block] = mixed.astype(jnp.bfloat16)
        copies.append(
            pltpu.make_async_copy(
                mixed_ref.at[block], out_hbm.at[:, columns(block, cols)], out_sem.at[block]
            )
        )
        copies[-1].start()
    for copy in copies:
        copy.wait()


def combine(table, back, gates, tokens):
    count, width = tokens.shape
    slots = back.shape[0]
    blocks = width // COMBINE_COLS
    return pl.pallas_call(
        combine_kernel,
        in_specs=[VMEM, VMEM, VMEM, VMEM],
        out_specs=HBM,
        out_shape=jax.ShapeDtypeStruct((count, width), jnp.bfloat16),
        scratch_shapes=[
            pltpu.VMEM((blocks, count, COMBINE_COLS), jnp.bfloat16),
            pltpu.SemaphoreType.DMA((blocks,)),
        ],
        compiler_params=pltpu.CompilerParams(vmem_limit_bytes=16 << 20),
        cost_estimate=pl.CostEstimate(
            flops=2 * slots * count * width, bytes_accessed=4 * slots * width, transcendentals=0
        ),
        name="combine",
    )(table, back, gates, tokens)


def exchange(rows, devices):
    parts = rows.reshape(devices, rows.shape[0] // devices, rows.shape[1])
    parts = lax.all_to_all(parts, ROW_COL, split_axis=0, concat_axis=0, tiled=True)
    return parts.reshape(rows.shape)


def on_device(tokens, expert_ids, gate_prob, norm_gain, weight_in, weight_out):
    tok_rows, width = tokens.shape
    experts = lax.axis_size(ROW_COL)
    slots = 2 * tok_rows
    tokens = pltpu.with_memory_space_constraint(tokens, pltpu.HBM)
    ids = pltpu.with_memory_space_constraint(expert_ids.reshape(1, tok_rows), pltpu.HBM)
    gain = pltpu.with_memory_space_constraint(norm_gain.reshape(1, width), pltpu.HBM)
    first = pltpu.with_memory_space_constraint(weight_in[0], pltpu.HBM)
    second = pltpu.with_memory_space_constraint(weight_out[0], pltpu.HBM)
    outgoing, placed, head = dispatch(tokens, ids, gain, first, slots)
    arrived = pltpu.with_memory_space_constraint(exchange(outgoing, experts), pltpu.VMEM)
    gate = gate_prob.reshape(1, tok_rows)
    answers, routed, table, gates, held = expert(
        arrived, head, placed, gate, first, second, tokens
    )
    returned = pltpu.with_memory_space_constraint(exchange(answers, experts), pltpu.VMEM)
    mixed = combine(table, returned, gates, held)
    return (mixed, routed)


def solution(mesh):
    finer = Mesh(mesh.devices.reshape(4, 2, 4, 4), ROW_COL)
    return jax.shard_map(
        on_device,
        mesh=finer,
        in_specs=(
            P(ROW_COL, None),
            P(ROW_COL, None),
            P(ROW_COL),
            P(),
            P(ROW_COL, None, None),
            P(ROW_COL, None, None),
        ),
        out_specs=(P(ROW_COL, None), P(ROW_COL)),
        check_vma=False,
    )
```

```python
import jax
import jax.numpy as jnp
from jax import lax
from jax.experimental import pallas as pl
from jax.experimental.pallas import tpu as pltpu
from jax.sharding import Mesh
from jax.sharding import PartitionSpec as P

ROW_COL = ("row_0", "row_1", "col_0", "col_1")
EMPTY = 32768.0
MARKED = 128
DISPATCH_COLS = 256
HEAD_COLS = 512
HIDDEN_COLS = 512
ANSWER_COLS = 512
COMBINE_COLS = 512
VMEM_LIMIT = 44 << 20

HBM = pl.BlockSpec(memory_space=pltpu.HBM)
VMEM = pl.BlockSpec(memory_space=pltpu.VMEM)
SMEM = pl.BlockSpec(memory_space=pltpu.SMEM)


def one_hot(match):
    return jnp.where(match, 1.0, 0.0).astype(jnp.bfloat16)


def columns(block, size, offset=0):
    start = block * size + offset
    return pl.ds(start if isinstance(block, int) else pl.multiple_of(start, 128), size)


def dispatch_kernel(
    tok_hbm, ids_hbm, gain_hbm, first_hbm, out_ref, placed_ref, head_ref,
    tok_ref, ids_ref, gain_ref, in_sem,
):
    count, width = tok_ref.shape
    slots, cols = out_ref.shape[0], DISPATCH_COLS
    experts = 128
    capacity = slots // experts
    ids_copy = pltpu.make_async_copy(ids_hbm, ids_ref, in_sem.at[0])
    tok_copy = pltpu.make_async_copy(tok_hbm, tok_ref, in_sem.at[1])
    gain_copy = pltpu.make_async_copy(gain_hbm, gain_ref, in_sem.at[2])
    ids_copy.start()
    tok_copy.start()
    gain_copy.start()
    head_copy = pltpu.make_async_copy(
        first_hbm.at[:, pl.ds(0, head_ref.shape[1])], head_ref, in_sem.at[3]
    )
    head_copy.start()
    before = lax.broadcasted_iota(jnp.int32, (count, count), 0) < lax.broadcasted_iota(
        jnp.int32, (count, count), 1
    )
    ids_copy.wait()
    ids = ids_ref[...]
    match = lax.broadcasted_iota(jnp.int32, (experts, count), 0) == ids
    earlier = jnp.dot(one_hot(match), one_hot(before), preferred_element_type=jnp.float32)
    within = jnp.sum(jnp.where(match, earlier, 0.0), axis=0, keepdims=True)
    placed = ids * capacity + within.astype(jnp.int32)
    placed_ref[...] = placed
    table = one_hot(lax.broadcasted_iota(jnp.int32, (slots, count), 0) == placed)
    filled = jnp.dot(
        table, jnp.ones((count, MARKED), jnp.bfloat16), preferred_element_type=jnp.float32
    )
    tok_copy.wait()
    gain_copy.wait()
    wide = tok_ref[...].astype(jnp.float32)
    scale = lax.rsqrt(jnp.mean(wide * wide, axis=1, keepdims=True) + 1e-06)
    normed = (wide * scale * gain_ref[...]).astype(jnp.bfloat16)
    for start in range(0, width, cols):
        sent = jnp.dot(
            table, normed[:, start : start + cols], preferred_element_type=jnp.float32
        )
        if start == 0:
            marked = jnp.where(filled > 0.5, sent[:, :MARKED], EMPTY).astype(jnp.bfloat16)
            out_ref[:, :MARKED] = marked
            out_ref[:, MARKED:cols] = sent[:, MARKED:].astype(jnp.bfloat16)
        else:
            out_ref[:, start : start + cols] = sent.astype(jnp.bfloat16)
    head_copy.wait()


def dispatch(tokens, ids, gain, first, slots):
    count, width = tokens.shape
    return pl.pallas_call(
        dispatch_kernel,
        in_specs=[HBM, HBM, HBM, HBM],
        out_specs=[VMEM, VMEM, VMEM],
        out_shape=[
            pltpu.VMEM((slots, width), jnp.bfloat16),
            jax.ShapeDtypeStruct((1, count), jnp.int32),
            pltpu.VMEM((first.shape[0], HEAD_COLS), jnp.bfloat16),
        ],
        scratch_shapes=[
            pltpu.VMEM((count, width), jnp.bfloat16),
            pltpu.VMEM((1, count), jnp.int32),
            pltpu.VMEM((1, width), jnp.float32),
            pltpu.SemaphoreType.DMA((4,)),
        ],
        compiler_params=pltpu.CompilerParams(vmem_limit_bytes=VMEM_LIMIT),
        cost_estimate=pl.CostEstimate(
            flops=2 * slots * count * width, bytes_accessed=4 * slots * width, transcendentals=0
        ),
        name="dispatch",
    )(tokens, ids, gain, first)


def expert_kernel(
    x_ref, head_ref, placed_ref, gate_ref, first_hbm, second_hbm, tok_hbm,
    out_ref, routed_ref, table_ref, gates_ref, tok_ref,
    first_ref, second_ref, hidden_ref, rows_ref, in_sem, tok_sem,
):
    hidden_blocks, _, hidden_cols = first_ref.shape
    answer_blocks, _, answer_cols = second_ref.shape
    head_cols = head_ref.shape[1]

    def first_copy(block):
        return pltpu.make_async_copy(
            first_hbm.at[:, columns(block, hidden_cols, head_cols)],
            first_ref.at[block],
            in_sem.at[0, block],
        )

    def second_copy(block):
        return pltpu.make_async_copy(
            second_hbm.at[:, columns(block, answer_cols)], second_ref.at[block], in_sem.at[1, block]
        )

    tok_copy = pltpu.make_async_copy(tok_hbm, tok_ref, tok_sem)
    for block in range(hidden_blocks):
        first_copy(block).start()
    for block in range(answer_blocks):
        second_copy(block).start()
    tok_copy.start()
    kept = jnp.where(x_ref[:, :MARKED].astype(jnp.float32) < 0.5 * EMPTY, 1.0, 0.0)
    routed_ref[0] = jnp.sum(kept).astype(jnp.int32) // MARKED

    count, lanes = rows_ref.shape
    placed = jnp.broadcast_to(placed_ref[...].astype(jnp.float32), (lanes, count))
    rows_ref[...] = placed.T.astype(jnp.int32)
    gates_ref[...] = jnp.broadcast_to(gate_ref[...], (lanes, count)).T

    def combine_columns(block):
        lane = lax.broadcasted_iota(jnp.int32, (count, lanes), 1) + block * lanes
        table_ref[:, columns(block, lanes)] = one_hot(lane == rows_ref[...])

    head = jnp.dot(x_ref[...], head_ref[...], preferred_element_type=jnp.float32)
    hidden_ref[:, :head_cols] = jnp.maximum(head, 0.0).astype(jnp.bfloat16)

    @pl.loop(0, hidden_blocks)
    def _(block):
        first_copy(block).wait()
        hidden = jnp.dot(x_ref[...], first_ref[block], preferred_element_type=jnp.float32)
        hidden_ref[:, columns(block, hidden_cols, head_cols)] = jnp.maximum(hidden, 0.0).astype(
            jnp.bfloat16
        )

    @pl.loop(0, answer_blocks)
    def _(block):
        second_copy(block).wait()
        steps = table_ref.shape[1] // lanes // answer_blocks
        for step in range(steps):
            combine_columns(block * steps + step)
        answer = jnp.dot(hidden_ref[...], second_ref[block], preferred_element_type=jnp.float32)
        out_ref[:, columns(block, answer_cols)] = answer.astype(jnp.bfloat16)

    tok_copy.wait()


def expert(x, head, placed, gate, first, second, tokens):
    rows, width = x.shape
    ff = first.shape[1]
    hidden_blocks, answer_blocks = (ff - HEAD_COLS) // HIDDEN_COLS, width // ANSWER_COLS
    return pl.pallas_call(
        expert_kernel,
        in_specs=[VMEM, VMEM, VMEM, VMEM, HBM, HBM, HBM],
        out_specs=[VMEM, SMEM, VMEM, VMEM, VMEM],
        out_shape=[
            pltpu.VMEM((rows, width), jnp.bfloat16),
            jax.ShapeDtypeStruct((1,), jnp.int32),
            pltpu.VMEM((placed.shape[1], rows), jnp.bfloat16),
            pltpu.VMEM((placed.shape[1], 128), jnp.float32),
            pltpu.VMEM(tokens.shape, jnp.bfloat16),
        ],
        scratch_shapes=[
            pltpu.VMEM((hidden_blocks, width, HIDDEN_COLS), jnp.bfloat16),
            pltpu.VMEM((answer_blocks, ff, ANSWER_COLS), jnp.bfloat16),
            pltpu.VMEM((rows, ff), jnp.bfloat16),
            pltpu.VMEM((placed.shape[1], 128), jnp.int32),
            pltpu.SemaphoreType.DMA((2, max(hidden_blocks, answer_blocks))),
            pltpu.SemaphoreType.DMA,
        ],
        compiler_params=pltpu.CompilerParams(vmem_limit_bytes=VMEM_LIMIT),
        cost_estimate=pl.CostEstimate(
            flops=4 * rows * width * ff, bytes_accessed=4 * width * (ff + rows), transcendentals=0
        ),
        name="expert",
    )(x, head, placed, gate, first, second, tokens)


def combine_kernel(
    table_ref, back_ref, gates_ref, tok_ref, out_hbm, mixed_ref, out_sem
):
    blocks, _, cols = mixed_ref.shape
    gates = jnp.concatenate([gates_ref[...]] * (cols // gates_ref.shape[1]), axis=1)
    copies = []
    for block in range(blocks):
        span = slice(block * cols, (block + 1) * cols)
        back = jnp.dot(table_ref[...], back_ref[:, span], preferred_element_type=jnp.float32)
        mixed = tok_ref[:, span].astype(jnp.float32) + gates * back
        mixed_ref[block] = mixed.astype(jnp.bfloat16)
        copies.append(
            pltpu.make_async_copy(
                mixed_ref.at[block], out_hbm.at[:, columns(block, cols)], out_sem.at[block]
            )
        )
        copies[-1].start()
    for copy in copies:
        copy.wait()


def combine(table, back, gates, tokens):
    count, width = tokens.shape
    slots = back.shape[0]
    blocks = width // COMBINE_COLS
    return pl.pallas_call(
        combine_kernel,
        in_specs=[VMEM, VMEM, VMEM, VMEM],
        out_specs=HBM,
        out_shape=jax.ShapeDtypeStruct((count, width), jnp.bfloat16),
        scratch_shapes=[
            pltpu.VMEM((blocks, count, COMBINE_COLS), jnp.bfloat16),
            pltpu.SemaphoreType.DMA((blocks,)),
        ],
        compiler_params=pltpu.CompilerParams(vmem_limit_bytes=16 << 20),
        cost_estimate=pl.CostEstimate(
            flops=2 * slots * count * width, bytes_accessed=4 * slots * width, transcendentals=0
        ),
        name="combine",
    )(table, back, gates, tokens)


def exchange(rows, devices):
    parts = rows.reshape(devices, rows.shape[0] // devices, rows.shape[1])
    parts = lax.all_to_all(parts, ROW_COL, split_axis=0, concat_axis=0, tiled=True)
    return parts.reshape(rows.shape)


def on_device(tokens, expert_ids, gate_prob, norm_gain, weight_in, weight_out):
    tok_rows, width = tokens.shape
    experts = lax.axis_size(ROW_COL)
    slots = 2 * tok_rows
    tokens = pltpu.with_memory_space_constraint(tokens, pltpu.HBM)
    ids = pltpu.with_memory_space_constraint(expert_ids.reshape(1, tok_rows), pltpu.HBM)
    gain = pltpu.with_memory_space_constraint(norm_gain.reshape(1, width), pltpu.HBM)
    first = pltpu.with_memory_space_constraint(weight_in[0], pltpu.HBM)
    second = pltpu.with_memory_space_constraint(weight_out[0], pltpu.HBM)
    outgoing, placed, head = dispatch(tokens, ids, gain, first, slots)
    arrived = pltpu.with_memory_space_constraint(exchange(outgoing, experts), pltpu.VMEM)
    gate = gate_prob.reshape(1, tok_rows)
    answers, routed, table, gates, held = expert(
        arrived, head, placed, gate, first, second, tokens
    )
    returned = pltpu.with_memory_space_constraint(exchange(answers, experts), pltpu.VMEM)
    mixed = combine(table, returned, gates, held)
    return (mixed, routed)


def solution(mesh):
    finer = Mesh(mesh.devices.reshape(4, 2, 4, 4), ROW_COL)
    return jax.shard_map(
        on_device,
        mesh=finer,
        in_specs=(
            P(ROW_COL, None),
            P(ROW_COL, None),
            P(ROW_COL),
            P(),
            P(ROW_COL, None, None),
            P(ROW_COL, None, None),
        ),
        out_specs=(P(ROW_COL, None), P(ROW_COL)),
        check_vma=False,
    )
```

```python
import jax
import jax.numpy as jnp
from jax import lax
from jax.experimental import pallas as pl
from jax.experimental.pallas import tpu as pltpu
from jax.sharding import Mesh
from jax.sharding import PartitionSpec as P

ROW_COL = ("row_0", "row_1", "col_0", "col_1")
EMPTY = 32768.0
MARKED = 128
DISPATCH_COLS = 256
HEAD_COLS = 512
HIDDEN_COLS = 512
ANSWER_COLS = 512
COMBINE_COLS = 512
VMEM_LIMIT = 44 << 20

HBM = pl.BlockSpec(memory_space=pltpu.HBM)
VMEM = pl.BlockSpec(memory_space=pltpu.VMEM)
SMEM = pl.BlockSpec(memory_space=pltpu.SMEM)


def one_hot(match):
    return jnp.where(match, 1.0, 0.0).astype(jnp.bfloat16)


def columns(block, size, offset=0):
    start = block * size + offset
    return pl.ds(start if isinstance(block, int) else pl.multiple_of(start, 128), size)


def dispatch_kernel(
    tok_hbm, ids_hbm, gain_hbm, first_hbm, out_ref, placed_ref, head_ref,
    tok_ref, ids_ref, gain_ref, in_sem,
):
    count, width = tok_ref.shape
    slots, cols = out_ref.shape[0], DISPATCH_COLS
    experts = 128
    capacity = slots // experts
    ids_copy = pltpu.make_async_copy(ids_hbm, ids_ref, in_sem.at[0])
    tok_copy = pltpu.make_async_copy(tok_hbm, tok_ref, in_sem.at[1])
    gain_copy = pltpu.make_async_copy(gain_hbm, gain_ref, in_sem.at[2])
    ids_copy.start()
    tok_copy.start()
    gain_copy.start()
    head_copy = pltpu.make_async_copy(
        first_hbm.at[:, pl.ds(0, head_ref.shape[1])], head_ref, in_sem.at[3]
    )
    head_copy.start()
    before = lax.broadcasted_iota(jnp.int32, (count, count), 0) < lax.broadcasted_iota(
        jnp.int32, (count, count), 1
    )
    ids_copy.wait()
    ids = ids_ref[...]
    match = lax.broadcasted_iota(jnp.int32, (experts, count), 0) == ids
    earlier = jnp.dot(one_hot(match), one_hot(before), preferred_element_type=jnp.float32)
    within = jnp.sum(jnp.where(match, earlier, 0.0), axis=0, keepdims=True)
    placed = ids * capacity + within.astype(jnp.int32)
    placed_ref[...] = placed
    table = one_hot(lax.broadcasted_iota(jnp.int32, (slots, count), 0) == placed)
    taken = jnp.dot(
        one_hot(match), jnp.ones((count, MARKED), jnp.bfloat16), preferred_element_type=jnp.float32
    )
    slot = lax.broadcasted_iota(jnp.int32, (experts, capacity, MARKED), 1).astype(jnp.float32)
    filled = jnp.where(slot < taken[:, None, :], 1.0, 0.0).reshape(slots, MARKED)
    tok_copy.wait()
    gain_copy.wait()
    wide = tok_ref[...].astype(jnp.float32)
    scale = lax.rsqrt(jnp.mean(wide * wide, axis=1, keepdims=True) + 1e-06)
    normed = (wide * scale * gain_ref[...]).astype(jnp.bfloat16)
    for start in range(0, width, cols):
        sent = jnp.dot(
            table, normed[:, start : start + cols], preferred_element_type=jnp.float32
        )
        if start == 0:
            marked = jnp.where(filled > 0.5, sent[:, :MARKED], EMPTY).astype(jnp.bfloat16)
            out_ref[:, :MARKED] = marked
            out_ref[:, MARKED:cols] = sent[:, MARKED:].astype(jnp.bfloat16)
        else:
            out_ref[:, start : start + cols] = sent.astype(jnp.bfloat16)
    head_copy.wait()


def dispatch(tokens, ids, gain, first, slots):
    count, width = tokens.shape
    return pl.pallas_call(
        dispatch_kernel,
        in_specs=[HBM, HBM, HBM, HBM],
        out_specs=[VMEM, VMEM, VMEM],
        out_shape=[
            pltpu.VMEM((slots, width), jnp.bfloat16),
            jax.ShapeDtypeStruct((1, count), jnp.int32),
            pltpu.VMEM((first.shape[0], HEAD_COLS), jnp.bfloat16),
        ],
        scratch_shapes=[
            pltpu.VMEM((count, width), jnp.bfloat16),
            pltpu.VMEM((1, count), jnp.int32),
            pltpu.VMEM((1, width), jnp.float32),
            pltpu.SemaphoreType.DMA((4,)),
        ],
        compiler_params=pltpu.CompilerParams(vmem_limit_bytes=VMEM_LIMIT),
        cost_estimate=pl.CostEstimate(
            flops=2 * slots * count * width, bytes_accessed=4 * slots * width, transcendentals=0
        ),
        name="dispatch",
    )(tokens, ids, gain, first)


def expert_kernel(
    x_ref, head_ref, placed_ref, gate_ref, first_hbm, second_hbm, tok_hbm,
    out_ref, routed_ref, table_ref, gates_ref, tok_ref,
    first_ref, second_ref, hidden_ref, rows_ref, in_sem, tok_sem,
):
    hidden_blocks, _, hidden_cols = first_ref.shape
    answer_blocks, _, answer_cols = second_ref.shape
    head_cols = head_ref.shape[1]

    def first_copy(block):
        return pltpu.make_async_copy(
            first_hbm.at[:, columns(block, hidden_cols, head_cols)],
            first_ref.at[block],
            in_sem.at[0, block],
        )

    def second_copy(block):
        return pltpu.make_async_copy(
            second_hbm.at[:, columns(block, answer_cols)], second_ref.at[block], in_sem.at[1, block]
        )

    tok_copy = pltpu.make_async_copy(tok_hbm, tok_ref, tok_sem)
    for block in range(hidden_blocks):
        first_copy(block).start()
    for block in range(answer_blocks):
        second_copy(block).start()
    tok_copy.start()
    kept = jnp.where(x_ref[:, :MARKED].astype(jnp.float32) < 0.5 * EMPTY, 1.0, 0.0)
    routed_ref[0] = jnp.sum(kept).astype(jnp.int32) // MARKED

    count, lanes = rows_ref.shape
    placed = jnp.broadcast_to(placed_ref[...].astype(jnp.float32), (lanes, count))
    rows_ref[...] = placed.T.astype(jnp.int32)
    gates_ref[...] = jnp.broadcast_to(gate_ref[...], (lanes, count)).T

    def combine_columns(block):
        lane = lax.broadcasted_iota(jnp.int32, (count, lanes), 1) + block * lanes
        table_ref[:, columns(block, lanes)] = one_hot(lane == rows_ref[...])

    head = jnp.dot(x_ref[...], head_ref[...], preferred_element_type=jnp.float32)
    hidden_ref[:, :head_cols] = jnp.maximum(head, 0.0).astype(jnp.bfloat16)

    @pl.loop(0, hidden_blocks)
    def _(block):
        first_copy(block).wait()
        hidden = jnp.dot(x_ref[...], first_ref[block], preferred_element_type=jnp.float32)
        hidden_ref[:, columns(block, hidden_cols, head_cols)] = jnp.maximum(hidden, 0.0).astype(
            jnp.bfloat16
        )

    @pl.loop(0, answer_blocks)
    def _(block):
        second_copy(block).wait()
        steps = table_ref.shape[1] // lanes // answer_blocks
        for step in range(steps):
            combine_columns(block * steps + step)
        answer = jnp.dot(hidden_ref[...], second_ref[block], preferred_element_type=jnp.float32)
        out_ref[:, columns(block, answer_cols)] = answer.astype(jnp.bfloat16)

    tok_copy.wait()


def expert(x, head, placed, gate, first, second, tokens):
    rows, width = x.shape
    ff = first.shape[1]
    hidden_blocks, answer_blocks = (ff - HEAD_COLS) // HIDDEN_COLS, width // ANSWER_COLS
    return pl.pallas_call(
        expert_kernel,
        in_specs=[VMEM, VMEM, VMEM, VMEM, HBM, HBM, HBM],
        out_specs=[VMEM, SMEM, VMEM, VMEM, VMEM],
        out_shape=[
            pltpu.VMEM((rows, width), jnp.bfloat16),
            jax.ShapeDtypeStruct((1,), jnp.int32),
            pltpu.VMEM((placed.shape[1], rows), jnp.bfloat16),
            pltpu.VMEM((placed.shape[1], 128), jnp.float32),
            pltpu.VMEM(tokens.shape, jnp.bfloat16),
        ],
        scratch_shapes=[
            pltpu.VMEM((hidden_blocks, width, HIDDEN_COLS), jnp.bfloat16),
            pltpu.VMEM((answer_blocks, ff, ANSWER_COLS), jnp.bfloat16),
            pltpu.VMEM((rows, ff), jnp.bfloat16),
            pltpu.VMEM((placed.shape[1], 128), jnp.int32),
            pltpu.SemaphoreType.DMA((2, max(hidden_blocks, answer_blocks))),
            pltpu.SemaphoreType.DMA,
        ],
        compiler_params=pltpu.CompilerParams(vmem_limit_bytes=VMEM_LIMIT),
        cost_estimate=pl.CostEstimate(
            flops=4 * rows * width * ff, bytes_accessed=4 * width * (ff + rows), transcendentals=0
        ),
        name="expert",
    )(x, head, placed, gate, first, second, tokens)


def combine_kernel(
    table_ref, back_ref, gates_ref, tok_ref, out_hbm, mixed_ref, out_sem
):
    blocks, _, cols = mixed_ref.shape
    gates = jnp.concatenate([gates_ref[...]] * (cols // gates_ref.shape[1]), axis=1)
    copies = []
    for block in range(blocks):
        span = slice(block * cols, (block + 1) * cols)
        back = jnp.dot(table_ref[...], back_ref[:, span], preferred_element_type=jnp.float32)
        mixed = tok_ref[:, span].astype(jnp.float32) + gates * back
        mixed_ref[block] = mixed.astype(jnp.bfloat16)
        copies.append(
            pltpu.make_async_copy(
                mixed_ref.at[block], out_hbm.at[:, columns(block, cols)], out_sem.at[block]
            )
        )
        copies[-1].start()
    for copy in copies:
        copy.wait()


def combine(table, back, gates, tokens):
    count, width = tokens.shape
    slots = back.shape[0]
    blocks = width // COMBINE_COLS
    return pl.pallas_call(
        combine_kernel,
        in_specs=[VMEM, VMEM, VMEM, VMEM],
        out_specs=HBM,
        out_shape=jax.ShapeDtypeStruct((count, width), jnp.bfloat16),
        scratch_shapes=[
            pltpu.VMEM((blocks, count, COMBINE_COLS), jnp.bfloat16),
            pltpu.SemaphoreType.DMA((blocks,)),
        ],
        compiler_params=pltpu.CompilerParams(vmem_limit_bytes=16 << 20),
        cost_estimate=pl.CostEstimate(
            flops=2 * slots * count * width, bytes_accessed=4 * slots * width, transcendentals=0
        ),
        name="combine",
    )(table, back, gates, tokens)


def exchange(rows, devices):
    parts = rows.reshape(devices, rows.shape[0] // devices, rows.shape[1])
    parts = lax.all_to_all(parts, ROW_COL, split_axis=0, concat_axis=0, tiled=True)
    return parts.reshape(rows.shape)


def on_device(tokens, expert_ids, gate_prob, norm_gain, weight_in, weight_out):
    tok_rows, width = tokens.shape
    experts = lax.axis_size(ROW_COL)
    slots = 2 * tok_rows
    tokens = pltpu.with_memory_space_constraint(tokens, pltpu.HBM)
    ids = pltpu.with_memory_space_constraint(expert_ids.reshape(1, tok_rows), pltpu.HBM)
    gain = pltpu.with_memory_space_constraint(norm_gain.reshape(1, width), pltpu.HBM)
    first = pltpu.with_memory_space_constraint(weight_in[0], pltpu.HBM)
    second = pltpu.with_memory_space_constraint(weight_out[0], pltpu.HBM)
    outgoing, placed, head = dispatch(tokens, ids, gain, first, slots)
    arrived = pltpu.with_memory_space_constraint(exchange(outgoing, experts), pltpu.VMEM)
    gate = gate_prob.reshape(1, tok_rows)
    answers, routed, table, gates, held = expert(
        arrived, head, placed, gate, first, second, tokens
    )
    returned = pltpu.with_memory_space_constraint(exchange(answers, experts), pltpu.VMEM)
    mixed = combine(table, returned, gates, held)
    return (mixed, routed)


def solution(mesh):
    finer = Mesh(mesh.devices.reshape(4, 2, 4, 4), ROW_COL)
    return jax.shard_map(
        on_device,
        mesh=finer,
        in_specs=(
            P(ROW_COL, None),
            P(ROW_COL, None),
            P(ROW_COL),
            P(),
            P(ROW_COL, None, None),
            P(ROW_COL, None, None),
        ),
        out_specs=(P(ROW_COL, None), P(ROW_COL)),
        check_vma=False,
    )
```
